32 devices in a mesh: dp: 4 (over y, core), expert: 8 (over z, x).
Axes of the slice: x: 2, y: 2, z: 4, core: 2. Of those that a mesh axis runs over, the one named last changes fastest.
Arguments:
- tokens: bfloat16 [4, 4, 4096, 1024], P('dp', None, 'expert'), may hold values from -8000 to 8000
- slot_params: bfloat16 [1024, 128], replicated, may hold values from -8 to 8
- dest: int32 [4, 4, 16], P('dp', None, 'expert'), may hold values from 0 to 63, as said below
- lengths: int32 [4, 4], P('dp'), may hold values from 256 to 4096
- w_in: bfloat16 [64, 1024, 4096], P('expert', None, 'dp'), may hold values from -0.1875 to 0.1875
- w_out: bfloat16 [64, 4096, 1024], P('expert', 'dp'), may hold values from -3 to 3
Outputs:
- mixed: bfloat16 [4, 64, 256, 1024], P('dp', 'expert')
The draws below stay inside these ranges and needn't reach their ends.
Inputs may be any that keep to these rules, and one draw needn't show every extreme that they name: For each g, dest[g] holds every number of 0 to 63 once; the 8 blocks held by one device (block indices j from k * 2 on, for every q) go to output blocks of different devices, device d holding output blocks d * 4 * 2 onward, so each device receives at most one block from each device.
All inputs are finite; a program needn't handle non-finite values.
Results may differ from the reference program's by a relative error of at most 0.01.
Values may be sent and summed in bfloat16 or wider, within the bound.
A program may use at most 128 MiB of HBM per device.

```python
import math
import jax
import jax.numpy as jnp
from jax import lax

D = 1024
H = 4096
SLOTS = 2
BT = 256
SEQ_DP = 4
BLK_DEV = 2
EXPERTS = 64
GROUPS = 4
SHARDS = 8
LEN = 4096


def shared_columns(key):
    base = jax.random.normal(jax.random.fold_in(key, 11), (D, EXPERTS * SLOTS), jnp.float32) * (0.3 / math.sqrt(D))
    return base


def draw_slot_params(key, part):
    return shared_columns(key).astype(jnp.bfloat16)


def draw_tokens(key, part):
    slot_count = EXPERTS * SLOTS
    noise = jnp.clip(jax.random.normal(jax.random.fold_in(key, 21), (GROUPS, SEQ_DP, LEN, D), jnp.float32), -6.0, 6.0)
    peaked = jax.random.bernoulli(jax.random.fold_in(key, 24), 0.5, (GROUPS, SEQ_DP, LEN, 1))
    spread = jnp.where(peaked, 2.5, 5.0)
    columns = shared_columns(key).T
    norms = jnp.sum(columns * columns, axis=1)
    unit_columns = columns / norms[:, None]
    chosen = jax.random.randint(jax.random.fold_in(key, 25), (GROUPS, SEQ_DP, LEN), 0, slot_count)
    boost = 7.0 * jnp.take(unit_columns, chosen, axis=0)
    base = noise * spread + jnp.where(peaked, boost, 0.0)
    return base.astype(jnp.bfloat16)


def draw_w_out(key, part):
    common = jnp.clip(jax.random.normal(jax.random.fold_in(key, 41), (H, D), jnp.float32), -5.0, 5.0) * (4.0 / math.sqrt(H))
    own = jnp.clip(jax.random.normal(jax.random.fold_in(key, 42), (EXPERTS, H, D), jnp.float32), -5.0, 5.0) * (1.0 / math.sqrt(H))
    return (common[None, :, :] + own).astype(jnp.bfloat16)


def draw_dest(key, part):
    per_device = SEQ_DP * BLK_DEV
    group_keys = jax.random.split(jax.random.fold_in(key, 31), GROUPS)
    shifts = jax.vmap(lambda k: jax.random.permutation(k, SHARDS)[:per_device])(group_keys).astype(jnp.int32)
    source_keys = jax.random.split(jax.random.fold_in(key, 32), GROUPS * SHARDS)
    source_order = jax.vmap(lambda k: jax.random.permutation(k, per_device))(source_keys).reshape(GROUPS, SHARDS, per_device).astype(jnp.int32)
    target_keys = jax.random.split(jax.random.fold_in(key, 33), GROUPS * SHARDS)
    target_order = jax.vmap(lambda k: jax.random.permutation(k, per_device))(target_keys).reshape(GROUPS, SHARDS, per_device).astype(jnp.int32)
    sources = jnp.arange(SHARDS, dtype=jnp.int32)
    receiver = (sources[None, :, None] + shifts[:, None, :]) % SHARDS
    group_index = jnp.arange(GROUPS, dtype=jnp.int32)[:, None, None]
    within = target_order[group_index, receiver, jnp.arange(per_device, dtype=jnp.int32)[None, None, :]]
    values = receiver * per_device + within
    table = jnp.zeros((GROUPS, SHARDS, per_device), jnp.int32)
    table = table.at[group_index, sources[None, :, None], source_order].set(values)
    table = table.reshape(GROUPS, SHARDS, SEQ_DP, BLK_DEV).transpose(0, 2, 1, 3)
    return table.reshape(GROUPS, SEQ_DP, SHARDS * BLK_DEV).astype(jnp.int32)


def place_ends(entries, stream_key, least, top_value):
    dims = entries.shape
    place = [jax.random.randint(jax.random.fold_in(stream_key, axis), (), 0, dims[axis]) for axis in range(len(dims))]
    entries = entries.at[tuple(place)].set(least)
    longest = dims.index(max(dims))
    place[longest] = (place[longest] + 1) % dims[longest]
    return entries.at[tuple(place)].set(top_value)


def block_levels(rng, shape, cuts, smallest, high):
    def one(axis_at, blocks):
        steps = jax.random.uniform(jax.random.fold_in(jax.random.fold_in(rng, 6), axis_at), (blocks,), jnp.float32, smallest / len(cuts), high / len(cuts))
        return jnp.repeat(jnp.exp(steps), shape[axis_at] // blocks).reshape((-1,) + (1,) * (len(shape) - axis_at - 1))

    loudness = one(*cuts[0])
    for cut in cuts[1:]:
        loudness = loudness * one(*cut)
    return loudness


def normal_values(key, shape, scale, limit, cuts=(), kind=jnp.bfloat16):
    values = scale * jax.random.normal(key, shape, jnp.float32)
    if cuts:
        values = values * block_levels(key, shape, cuts, -0.22, 0.18)
    return jnp.clip(values, -limit, limit).astype(kind)


def setup_inputs(seed: int = 0) -> dict:
    key_list = jax.random.split(jax.random.key(seed), 7)
    tokens = draw_tokens(jax.random.fold_in(key_list[6], 71), 0)
    slot_params = draw_slot_params(jax.random.fold_in(key_list[6], 71), 0)
    dest = draw_dest(jax.random.fold_in(key_list[6], 71), 0)
    lengths = place_ends(jax.random.randint(key_list[3], (GROUPS, SEQ_DP), BT, LEN + 1), jax.random.fold_in(key_list[3], 1), BT, LEN).astype(jnp.int32)
    w_in = normal_values(key_list[4], (EXPERTS, D, H), D ** -0.5, 0.1875, ((0, 8), (2, 4)))
    w_out = draw_w_out(jax.random.fold_in(key_list[6], 71), 0)
    return {"tokens": tokens, "slot_params": slot_params, "dest": dest, "lengths": lengths, "w_in": w_in, "w_out": w_out}


def reference(tokens, slot_params, dest, lengths, w_in, w_out):
    groups, seqs, length, width = tokens.shape
    slots_total = slot_params.shape[1]
    experts = w_in.shape[0]
    per_expert = slots_total // experts
    block_count = length // BT
    position = jnp.arange(length, dtype=jnp.int32)
    flat_tokens = tokens.reshape(groups * seqs, length, width)
    flat_lengths = lengths.reshape(groups * seqs).astype(jnp.int32)

    def dispatch(args):
        feats, count = args
        live_mask = position < count
        logits = jnp.dot(feats, slot_params, preferred_element_type=jnp.float32)
        masked = jnp.where(live_mask[:, None], logits, -jnp.inf)
        top = jnp.max(masked, axis=0)
        weight = jnp.where(live_mask[:, None], jnp.exp(logits - top[None, :]), 0.0)
        mass = jnp.sum(weight, axis=0)
        numer = jnp.dot(weight.astype(jnp.bfloat16).T, feats, preferred_element_type=jnp.float32)
        return (numer / mass[:, None]).astype(jnp.bfloat16)

    slot_in = lax.map(dispatch, (flat_tokens, flat_lengths))
    by_expert = slot_in.reshape(groups * seqs, experts, per_expert, width)
    by_expert = by_expert.transpose(1, 0, 2, 3).reshape(experts, groups * seqs * per_expert, width)

    def expert_apply(args):
        rows_in, first, second = args
        hidden = jax.nn.gelu(jnp.dot(rows_in, first, preferred_element_type=jnp.float32)).astype(jnp.bfloat16)
        return jnp.dot(hidden, second, preferred_element_type=jnp.float32).astype(jnp.bfloat16)

    expert_rows = lax.map(expert_apply, (by_expert, w_in, w_out))
    slot_out = expert_rows.reshape(experts, groups * seqs, per_expert, width)
    slot_out = slot_out.transpose(1, 0, 2, 3).reshape(groups * seqs, slots_total, width)

    def combine(args):
        feats, count, outputs = args
        live_mask = position < count
        logits = jnp.dot(feats, slot_params, preferred_element_type=jnp.float32)
        mix = jax.nn.softmax(logits, axis=1).astype(jnp.bfloat16)
        result = jnp.dot(mix, outputs, preferred_element_type=jnp.float32)
        return jnp.where(live_mask[:, None], result, 0.0).astype(jnp.bfloat16)

    combined = lax.map(combine, (flat_tokens, flat_lengths, slot_out))
    blocks = combined.reshape(groups, seqs * block_count, BT, width)
    order = dest.reshape(groups, seqs * block_count).astype(jnp.int32)
    group_index = jnp.arange(groups, dtype=jnp.int32)[:, None]
    mixed = jnp.zeros_like(blocks).at[group_index, order].set(blocks)
    return mixed
```

```python
import functools

import jax
import jax.numpy as jnp
from jax import lax
from jax.experimental import pallas as pl
from jax.experimental.pallas import tpu as pltpu
from jax.sharding import PartitionSpec as P

LANES = 128
FLOOR = -3.0e38
GATHER_BYTES = 512 * 1024


def pieces(value):
    high = lax.reduce_precision(value, 8, 7)
    rest = value - high
    middle = lax.reduce_precision(rest, 8, 7)
    return [high, middle, rest - middle]


def combine_kernel(order, seq_of, mix_ref, *refs):
    out_ref = refs[-1]
    start = 0
    for ref in refs[:-1]:
        shards, _, owned, columns = ref.shape
        outputs = ref[...].reshape(shards * owned, columns)
        out_ref[0, :, start : start + columns] = jnp.dot(
            mix_ref[0], outputs, preferred_element_type=jnp.float32
        ).astype(out_ref.dtype)
        start += columns


def combine(order, seq_of, mixes, outputs, held_blocks, block_tokens):
    slots_total = mixes.shape[2]
    width = sum(part.shape[3] for part in outputs)
    specs = [
        pl.BlockSpec((1, block_tokens, slots_total), lambda o, order, seq: (order[o], 0, 0))
    ]
    for part in outputs:
        specs.append(
            pl.BlockSpec(
                (part.shape[0], 1, part.shape[2], part.shape[3]),
                lambda o, order, seq: (0, seq[o], 0, 0),
            )
        )
    return pl.pallas_call(
        combine_kernel,
        grid_spec=pltpu.PrefetchScalarGridSpec(
            num_scalar_prefetch=2,
            grid=(held_blocks,),
            in_specs=specs,
            out_specs=pl.BlockSpec((1, block_tokens, width), lambda o, order, seq: (o, 0, 0)),
        ),
        out_shape=jax.ShapeDtypeStruct((held_blocks, block_tokens, width), jnp.bfloat16),
    )(order, seq_of, mixes, *outputs)


def local(tokens, slot_params, dest, lengths, w_in, w_out):
    seq_count = tokens.shape[1]
    tokens_here = tokens.shape[2]
    width = tokens.shape[3]
    blocks_here = dest.shape[2]
    block_tokens = tokens_here // blocks_here
    held_blocks = seq_count * blocks_here
    shard_count = lax.axis_size("expert")
    group_count = lax.axis_size("dp")
    shard_index = lax.axis_index("expert")
    slots_total = slot_params.shape[1]
    owned_slots = slots_total // shard_count
    feats = tokens[0]
    place = shard_index * tokens_here + jnp.arange(tokens_here, dtype=jnp.int32)
    live = (place[None, :] < lengths[0][:, None])[..., None]

    logits = jnp.dot(
        feats.reshape(seq_count * tokens_here, width),
        slot_params,
        preferred_element_type=jnp.float32,
    ).reshape(seq_count, tokens_here, slots_total)

    top = jnp.maximum(jnp.max(jnp.where(live, logits, -jnp.inf), axis=1), FLOOR)
    weight = jnp.where(live, jnp.exp(logits - top[:, None, :]), 0.0)
    mass = jnp.sum(weight, axis=1)
    numer = jnp.einsum(
        "qts,qtd->qsd", weight.astype(jnp.bfloat16), feats, preferred_element_type=jnp.float32
    ).astype(jnp.bfloat16)
    extra = jnp.stack(pieces(top) + pieces(mass), axis=-1).astype(jnp.bfloat16)
    extra = jnp.pad(extra, ((0, 0), (0, 0), (0, LANES - extra.shape[-1])))
    packed = jnp.concatenate([numer, extra], axis=-1)
    packed = packed.reshape(seq_count, shard_count, owned_slots, width + LANES)
    packed = lax.all_to_all(packed.transpose(1, 0, 2, 3), "expert", 0, 0, tiled=True)
    stats = packed[..., width : width + 6].astype(jnp.float32)
    tops = stats[..., 0] + stats[..., 1] + stats[..., 2]
    masses = stats[..., 3] + stats[..., 4] + stats[..., 5]
    scale = jnp.exp(tops - jnp.max(tops, axis=0, keepdims=True))
    mass_own = jnp.sum(scale * masses, axis=0)
    numer_own = jnp.sum(scale[..., None] * packed[..., :width].astype(jnp.float32), axis=0)
    slot_in = (numer_own / mass_own[..., None]).astype(jnp.bfloat16)

    mix = jnp.where(live, jax.nn.softmax(logits, axis=-1), 0.0).astype(jnp.bfloat16)
    mix = mix.reshape(held_blocks, block_tokens, slots_total)
    targets = dest.reshape(held_blocks)
    ordinal = jnp.arange(held_blocks, dtype=jnp.int32)
    shards = jnp.arange(shard_count, dtype=jnp.int32)
    goes = (targets // held_blocks)[None, :] == shards[:, None]
    pick = jnp.sum(jnp.where(goes, ordinal[None, :], 0), axis=1)
    label = jnp.sum(jnp.where(goes, (targets % held_blocks + 1)[None, :], 0), axis=1) - 1
    sender_seq = pick // blocks_here
    note = jnp.stack([label, sender_seq], axis=-1).astype(jnp.bfloat16)
    note = jnp.pad(note, ((0, 0), (0, slots_total - 2)))
    note = jnp.broadcast_to(note[:, None, :], (shard_count, 16, slots_total))
    outgoing = jnp.concatenate([mix[pick], note], axis=1)
    mixes = lax.all_to_all(outgoing, "expert", 0, 0, tiled=True)
    labels = mixes[:, block_tokens, 0].astype(jnp.int32)
    seqs = mixes[:, block_tokens, 1].astype(jnp.int32)
    comes = labels[None, :] == ordinal[:, None]
    order = jnp.sum(jnp.where(comes, shards[None, :], 0), axis=1)
    order_seq = jnp.sum(jnp.where(comes, seqs[None, :], 0), axis=1)

    gathered = lax.all_gather(slot_in, "dp", axis=0, tiled=True)
    experts_here = w_in.shape[0]
    per_expert = owned_slots // experts_here
    grouped = gathered.reshape(gathered.shape[0], experts_here, per_expert, width)
    hidden = jax.nn.gelu(
        jnp.einsum("nepd,edh->neph", grouped, w_in, preferred_element_type=jnp.float32)
    ).astype(jnp.bfloat16)
    result = jnp.einsum("neph,ehd->nepd", hidden, w_out, preferred_element_type=jnp.float32)
    partial = result.astype(jnp.bfloat16).reshape(
        group_count, seq_count, owned_slots, width
    )
    partial = lax.all_to_all(partial, "dp", 0, 0, tiled=True)
    slot_out = jnp.sum(partial.astype(jnp.float32), axis=0).astype(jnp.bfloat16)

    chunks = 1
    while seq_count * slots_total * width * 2 // chunks > GATHER_BYTES:
        chunks *= 2
    step = width // chunks
    outputs = [
        lax.all_gather(slot_out[..., c * step : (c + 1) * step], "expert", axis=0)
        for c in range(chunks)
    ]
    mixed = combine(order, order_seq, mixes, outputs, held_blocks, block_tokens)
    return mixed[None]


def solution(mesh):
    return jax.shard_map(
        local,
        mesh=mesh,
        in_specs=(
            P("dp", None, "expert", None),
            P(),
            P("dp", None, "expert"),
            P("dp", None),
            P("expert", None, "dp"),
            P("expert", "dp", None),
        ),
        out_specs=P("dp", "expert", None, None),
        check_vma=False,
    )
```
